256 devices in a mesh: mem: 32 (over x, y, core), mp: 8 (over z).
Axes of the slice: x: 4, y: 4, z: 8, core: 2. Of those that a mesh axis runs over, the one named last changes fastest.
Arguments:
- queries: bfloat16 [12288, 4096], P('mem', 'mp'), may hold values from -5 to 5
- local_keys: bfloat16 [12288, 4096], P('mem', 'mp'), may hold values from -5 to 5
- local_values: bfloat16 [12288, 4096], P('mem', 'mp'), may hold values from -6 to 6
- memory_keys: bfloat16 [65536, 4096], P('mem', 'mp'), may hold values from -5 to 5
- memory_values: bfloat16 [65536, 4096], P('mem', 'mp'), may hold values from -6 to 6
- grad_out: bfloat16 [12288, 4096], P('mem'), may hold values from -6 to 6
- out_weight: bfloat16 [4096, 4096], P('mem', 'mp'), may hold values from -0.09375 to 0.09375
- gate_logits: float32 [32], P('mp'), may hold values from -2 to 2
- tile_ids: int32 [96, 32, 4], P('mem', 'mp'), may hold values from 0 to 511, as said below
- window: int32 [96], P('mem'), may hold values from 1 to 256, as said below
Outputs:
- grad_queries: bfloat16 [12288, 4096], P('mem', 'mp')
- grad_keys: bfloat16 [12288, 4096], P('mem', 'mp')
- grad_values: bfloat16 [12288, 4096], P('mem', 'mp')
The draws below stay inside these ranges and needn't reach their ends.
Inputs may be any that keep to these rules, and one draw needn't show every extreme that they name: `tile_ids`: owner of tile id t is t // 16. Among the 48 ids of the blocks and heads that one device holds (one index of mem and of mp), at most 3 name tiles of any one owner; in every draw one owner receives exactly 3 of them from every device. Ids of one block and head may repeat. `window`: 256 is taken by some block in every draw.
All inputs are finite; a program needn't handle non-finite values.
Results may differ from the reference program's by a relative error of at most 0.011.
Values may be sent and summed in bfloat16 or wider, within the bound.
No kernel may reach another device: no remote copies, remote signals or barrier semaphores. Data moves between devices by JAX's collectives and lax.ppermute only.
A program may use at most 128 MiB of HBM per device.

```python
import math
import jax
import jax.numpy as jnp
from jax import lax

D = 4096
HEADS = 32
DH = 128
BLK = 128
TOP = 4
WIN = 256
TOK_DEV = 384
TILES_DEV = 16
HEADS_DEV = 4
TOKENS = 12288
BLOCKS = 96
MEMROWS = 65536
RET_DEV = 48
CAP = 3
N_MEM = 32
N_MP = 8


def rough_rows(key, count):
    base_draw = jax.random.normal(key, (count, HEADS * DH), jnp.float32)
    return jnp.clip(base_draw, -4.0, 4.0)


def drawn_keys(key, count, salt):
    field_rows = rough_rows(jax.random.fold_in(key, salt), count)
    return field_rows


def draw_local_keys(key, part):
    return drawn_keys(key, TOKENS, 11).astype(jnp.bfloat16)


def draw_memory_keys(key, part):
    return drawn_keys(key, MEMROWS, 12).astype(jnp.bfloat16)


def draw_queries(key, part):
    field_rows = rough_rows(jax.random.fold_in(key, 13), TOKENS)
    return field_rows.astype(jnp.bfloat16)


def draw_tile_ids(key, part):
    groups = N_MEM * N_MP
    hot_owner = jax.random.randint(jax.random.fold_in(key, 21), (), 0, N_MEM)
    order_keys = jax.random.split(jax.random.fold_in(key, 22), groups)
    other_orders = jax.vmap(lambda group_key: jax.random.permutation(group_key, N_MEM - 1))(order_keys)
    place_keys = jax.random.split(jax.random.fold_in(key, 23), groups)
    placing = jax.vmap(lambda group_key: jax.random.permutation(group_key, RET_DEV))(place_keys)
    ranks = jnp.arange(RET_DEV)
    others = (hot_owner + 1 + other_orders) % N_MEM
    rest_index = jnp.maximum(ranks - CAP, 0) % (N_MEM - 1)
    by_rank = jnp.where(ranks[None, :] < CAP, hot_owner, others[:, rest_index])
    owner_ids = jnp.take_along_axis(by_rank, placing, axis=1)
    within = jax.random.randint(jax.random.fold_in(key, 24), (groups, RET_DEV), 0, TILES_DEV)
    tile_numbers = owner_ids * TILES_DEV + within
    tile_numbers = tile_numbers.reshape(N_MEM, N_MP, TOK_DEV // BLK, HEADS_DEV, TOP)
    return tile_numbers.transpose(0, 2, 1, 3, 4).reshape(BLOCKS, HEADS, TOP).astype(jnp.int32)


def draw_window(key, part):
    widths = jax.random.randint(jax.random.fold_in(key, 31), (BLOCKS,), 1, WIN + 1)
    chosen = jax.random.randint(jax.random.fold_in(key, 32), (), 0, BLOCKS)
    return jnp.where(jnp.arange(BLOCKS) == chosen, WIN, widths).astype(jnp.int32)


def block_scale(stream_key, dims, cuts, low, largest):
    level = 1.0
    for dim, blocks in cuts:
        draws = jax.random.uniform(jax.random.fold_in(jax.random.fold_in(stream_key, 6), dim), (blocks,), jnp.float32, low / len(cuts), largest / len(cuts))
        level = level * jnp.repeat(jnp.exp(draws), dims[dim] // blocks).reshape((-1,) + (1,) * (len(dims) - 1 - dim))
    return level


def noise(stream_key, shape, deviation, limit, pieces=(), kind=jnp.bfloat16):
    values = deviation * jax.random.normal(stream_key, shape, jnp.float32)
    if pieces:
        values = values * block_scale(stream_key, shape, pieces, -0.22, 0.18)
    return jnp.clip(values, -limit, limit).astype(kind)


def setup_inputs(seed: int = 0) -> dict:
    key_of = jax.random.split(jax.random.key(seed), 11)
    queries = draw_queries(jax.random.fold_in(key_of[10], 71), 0)
    local_keys = draw_local_keys(jax.random.fold_in(key_of[10], 71), 0)
    local_values = noise(key_of[2], (TOKENS, D), 1.0, 6.0, ((0, 32), (1, 8)))
    memory_keys = draw_memory_keys(jax.random.fold_in(key_of[10], 71), 0)
    memory_values = noise(key_of[4], (MEMROWS, D), 1.0, 6.0, ((0, 32), (1, 8)))
    grad_out = noise(key_of[5], (TOKENS, D), 1.0, 6.0, ((0, 32),))
    out_weight = noise(key_of[6], (D, D), D ** -0.5, 0.09375, ((0, 32), (1, 8)))
    gate_logits = jnp.clip(jax.random.uniform(key_of[7], (HEADS,), jnp.float32, -2.0, 2.0) * block_scale(key_of[7], (HEADS,), ((0, 8),), -0.4, 0.0), -2.0, 2.0)
    tile_ids = draw_tile_ids(jax.random.fold_in(key_of[10], 71), 0)
    window = draw_window(jax.random.fold_in(key_of[10], 71), 0)
    return {"queries": queries, "local_keys": local_keys, "local_values": local_values, "memory_keys": memory_keys, "memory_values": memory_values, "grad_out": grad_out, "out_weight": out_weight, "gate_logits": gate_logits, "tile_ids": tile_ids, "window": window}


def reference(queries, local_keys, local_values, memory_keys, memory_values, grad_out, out_weight, gate_logits, tile_ids, window):
    score_scale = 1.0 / math.sqrt(DH)
    head_grad = jnp.dot(grad_out, out_weight, preferred_element_type=jnp.float32)
    gate_cols = jnp.repeat(jax.nn.sigmoid(gate_logits), DH)
    grad_memory = (gate_cols * head_grad).astype(jnp.bfloat16)
    grad_local = ((1.0 - gate_cols) * head_grad).astype(jnp.bfloat16)
    mem_key4 = memory_keys.reshape(TILES_DEV * N_MEM, BLK, HEADS, DH)
    mem_val4 = memory_values.reshape(TILES_DEV * N_MEM, BLK, HEADS, DH)
    head_index = jnp.arange(HEADS, dtype=jnp.int32)[:, None]

    def memory_block(inputs):
        query_block, grad_block, block_ids = inputs
        keys_mem = mem_key4[block_ids, :, head_index, :].reshape(HEADS, TOP * BLK, DH).astype(jnp.float32)
        vals_mem = mem_val4[block_ids, :, head_index, :].reshape(HEADS, TOP * BLK, DH).astype(jnp.float32)
        scores = jnp.einsum('qhd,hkd->hqk', query_block.astype(jnp.float32), keys_mem) * score_scale
        probs = jax.nn.softmax(scores, axis=-1)
        dprobs = jnp.einsum('qhd,hkd->hqk', grad_block.astype(jnp.float32), vals_mem)
        delta = lax.optimization_barrier(jnp.sum(probs * dprobs, axis=-1, keepdims=True))
        dscores = probs * (dprobs - delta)
        return jnp.einsum('hqk,hkd->hqd', dscores, keys_mem) * score_scale
    query_blocks = queries.reshape(BLOCKS, BLK, HEADS, DH)
    grad_blocks = grad_memory.reshape(BLOCKS, BLK, HEADS, DH)
    memory_qgrad = lax.map(memory_block, (query_blocks, grad_blocks, tile_ids))
    memory_qgrad = memory_qgrad.transpose(0, 2, 1, 3).reshape(TOKENS, D)
    key_pad = jnp.concatenate([jnp.zeros((2 * BLK, D), jnp.bfloat16), local_keys], axis=0)
    val_pad = jnp.concatenate([jnp.zeros((2 * BLK, D), jnp.bfloat16), local_values], axis=0)

    def local_block(carry, block):
        key_acc, val_acc = carry
        start = (block * BLK).astype(jnp.int32)
        query_block = lax.dynamic_slice_in_dim(queries, start, BLK, 0).reshape(BLK, HEADS, DH).astype(jnp.float32)
        grad_block = lax.dynamic_slice_in_dim(grad_local, start, BLK, 0).reshape(BLK, HEADS, DH).astype(jnp.float32)
        key_block = lax.dynamic_slice_in_dim(key_pad, start, 3 * BLK, 0).reshape(3 * BLK, HEADS, DH).astype(jnp.float32)
        val_block = lax.dynamic_slice_in_dim(val_pad, start, 3 * BLK, 0).reshape(3 * BLK, HEADS, DH).astype(jnp.float32)
        query_pos = start + jnp.arange(BLK, dtype=jnp.int32)
        key_pos = start - 2 * BLK + jnp.arange(3 * BLK, dtype=jnp.int32)
        width_here = window[block]
        allowed = (key_pos[None, :] <= query_pos[:, None]) & (key_pos[None, :] > query_pos[:, None] - width_here) & (key_pos[None, :] >= 0)
        scores = jnp.einsum('qhd,khd->hqk', query_block, key_block) * score_scale
        scores = jnp.where(allowed[None], scores, -jnp.inf)
        probs = jax.nn.softmax(scores, axis=-1)
        probs16 = probs.astype(jnp.bfloat16).astype(jnp.float32)
        dprobs = jnp.einsum('qhd,khd->hqk', grad_block, val_block)
        delta = lax.optimization_barrier(jnp.sum(probs * dprobs, axis=-1, keepdims=True))
        dscores16 = (probs * (dprobs - delta)).astype(jnp.bfloat16).astype(jnp.float32)
        query_grad = jnp.einsum('hqk,khd->qhd', dscores16, key_block) * score_scale
        key_grad = jnp.einsum('hqk,qhd->khd', dscores16, query_block) * score_scale
        val_grad = jnp.einsum('hqk,qhd->khd', probs16, grad_block)
        key_acc = lax.dynamic_update_slice_in_dim(key_acc, lax.dynamic_slice_in_dim(key_acc, start, 3 * BLK, 0) + key_grad.reshape(3 * BLK, D), start, 0)
        val_acc = lax.dynamic_update_slice_in_dim(val_acc, lax.dynamic_slice_in_dim(val_acc, start, 3 * BLK, 0) + val_grad.reshape(3 * BLK, D), start, 0)
        return ((key_acc, val_acc), query_grad.reshape(BLK, D))
    zero_acc = jnp.zeros((TOKENS + 2 * BLK, D), jnp.float32)
    (key_acc, val_acc), local_qgrad = lax.scan(local_block, (zero_acc, zero_acc), jnp.arange(BLOCKS, dtype=jnp.int32))
    local_qgrad = local_qgrad.reshape(TOKENS, D)
    grad_queries = (memory_qgrad + local_qgrad).astype(jnp.bfloat16)
    grad_keys = key_acc[2 * BLK:].astype(jnp.bfloat16)
    grad_values = val_acc[2 * BLK:].astype(jnp.bfloat16)
    return (grad_queries, grad_keys, grad_values)
```

```python
import functools
import math

import jax
import jax.numpy as jnp
from jax import lax
from jax.experimental import pallas as pl
from jax.experimental.pallas import tpu as pltpu
from jax.sharding import PartitionSpec as P


BLK = 128
DH = 128
UNITS = 5
LANES = 128
FLAG = 8
LOG2E = 1.4426950408889634
BF16 = jnp.bfloat16
F32 = jnp.float32
ANY = pl.BlockSpec(memory_space=pl.ANY)
SMEM = pl.BlockSpec(memory_space=pltpu.SMEM)
VMEM = pl.BlockSpec(memory_space=pltpu.VMEM)


def dot_nt(a, b):
    return lax.dot_general(a, b, (((1,), (1,)), ((), ())), preferred_element_type=F32)


def dot_nn(a, b):
    return lax.dot_general(a, b, (((1,), (0,)), ((), ())), preferred_element_type=F32)


def dot_tn(a, b):
    return lax.dot_general(a, b, (((0,), (0,)), ((), ())), preferred_element_type=F32)


def request_kernel(ids, request, slots, filled):
    blocks, heads, top = ids.shape
    members = request.shape[0]

    def clear(chip, carry):
        filled[chip] = 0
        for lane in range(UNITS + 1):
            request[2 * chip, 0, lane] = -1
            request[2 * chip + 1, 0, lane] = -1
        return carry

    def enter(group, over):
        block, head = group // heads, group % heads
        for t in range(top):
            tile = ids[block, head, t]
            chip = tile >> 5
            place = filled[chip]
            filled[chip] = place + 1
            code = (tile & 31) * heads + head
            request[2 * chip, 0, place] = code
            request[2 * chip + 1, 0, place] = code
            slots[group * top + t] = chip * 8 + place
            over = jnp.maximum(over, place)
        return over

    def flag(member, over):
        request[member, 0, FLAG] = (over >= UNITS).astype(jnp.int32)
        return over

    lax.fori_loop(0, members // 2, clear, 0)
    over = lax.fori_loop(0, blocks * heads, enter, jnp.int32(0))
    lax.fori_loop(0, members, flag, over)


def requests(ids, members):
    return pl.pallas_call(
        request_kernel,
        out_shape=(
            jax.ShapeDtypeStruct((members, 1, LANES), jnp.int32),
            jax.ShapeDtypeStruct((ids.size,), jnp.int32),
        ),
        in_specs=[SMEM],
        out_specs=(SMEM, SMEM),
        scratch_shapes=[pltpu.SMEM((members // 2,), jnp.int32)],
        name="requests",
    )(ids)


def gather_kernel(first, units, codes, core, keys, vals, peer_keys, peer_vals, out, stage, taken, given):
    members = codes.shape[0]

    def take(source, code, place):
        row = pl.multiple_of(((code >> 2) & 15) * BLK, BLK)
        col = pl.multiple_of((code & 3) * DH, DH)
        tile = source.at[pl.ds(row, BLK), pl.ds(col, DH)]
        return pltpu.make_async_copy(tile, stage.at[place], taken.at[place])

    def give(place):
        return pltpu.make_async_copy(stage.at[place], out.at[place], given.at[place])

    def each(step):
        def member(dest, carry):
            for unit in range(units):
                code = codes[dest, 0, first + unit]

                @pl.when(code >= 0)
                def _():
                    step(code, dest * units + unit)

            return carry

        lax.fori_loop(0, members, member, 0)

    for c, own, peer in ((0, keys, peer_keys), (1, vals, peer_vals)):

        def fetch(code, place, c=c, own=own, peer=peer):
            @pl.when((code >> 6) == c)
            def _():
                take(own, code, place).start()

            @pl.when((code >> 6) != c)
            def _():
                take(peer, code, place).start()

        @pl.when(core[0] == c)
        def _():
            each(fetch)

    def pass_on(code, place):
        take(keys, code, place).wait()
        give(place).start()

    each(pass_on)
    each(lambda code, place: give(place).wait())


def gather_tiles(codes, core, keys, vals, peer_keys, peer_vals, first, units):
    count = codes.shape[0] * units
    return pl.pallas_call(
        functools.partial(gather_kernel, first, units),
        out_shape=jax.ShapeDtypeStruct((count, BLK, DH), BF16),
        in_specs=[SMEM, SMEM, ANY, ANY, ANY, ANY],
        out_specs=ANY,
        scratch_shapes=[
            pltpu.VMEM((count, BLK, DH), BF16),
            pltpu.SemaphoreType.DMA((count,)),
            pltpu.SemaphoreType.DMA((count,)),
        ],
        name="gather_tiles",
    )(codes, core, keys, vals, peer_keys, peer_vals)


def closing_kernel(gk, gv, back, gk_out, gv_out):
    rest = gk.shape[0] - 2 * BLK
    for i, own, out in ((0, gk, gk_out), (1, gv, gv_out)):
        out[:rest] = own[:rest].astype(BF16)
        out[rest:] = (own[rest:] + back[i].astype(F32)).astype(BF16)


def closing(gk, gv, back):
    return pl.pallas_call(
        closing_kernel,
        out_shape=(jax.ShapeDtypeStruct(gk.shape, BF16), jax.ShapeDtypeStruct(gv.shape, BF16)),
        in_specs=[VMEM, VMEM, VMEM],
        out_specs=(VMEM, VMEM),
        name="closing",
    )(gk, gv, back)


def memory_kernel(units, heads, top, scale, slots, tiles, q, gm, lq, out, kbuf, vbuf, sems):
    blocks = q.shape[0] // BLK

    def copies(r):
        slot = slots[r]
        base = (slot >> 3) * 2 * units + (slot & 7)
        rows = pl.ds(pl.multiple_of((r % top) * BLK, BLK), BLK)
        return (
            pltpu.make_async_copy(tiles.at[base], kbuf.at[r // top, rows], sems.at[2 * r]),
            pltpu.make_async_copy(tiles.at[base + units], vbuf.at[r // top, rows], sems.at[2 * r + 1]),
        )

    def issue(r, carry):
        for one in copies(r):
            one.start()
        return carry

    lax.fori_loop(0, blocks * heads * top, issue, 0)
    for b in range(blocks):
        rows = slice(b * BLK, (b + 1) * BLK)
        for r in range(b * heads * top, (b + 1) * heads * top):
            for one in copies(r):
                one.wait()
        for h in range(heads):
            cols = slice(h * DH, (h + 1) * DH)
            keys = kbuf[b * heads + h]
            scores = dot_nt(q[rows, cols], keys)
            peak = jnp.max(scores, axis=-1, keepdims=True)
            expo = jnp.exp2((scores - peak) * (scale * LOG2E))
            inverse = 1.0 / jnp.sum(expo, axis=-1, keepdims=True)
            dprobs = dot_nt(gm[rows, cols], vbuf[b * heads + h])
            delta = jnp.sum(expo * dprobs, axis=-1, keepdims=True) * inverse
            dscores = (expo * (dprobs - delta)).astype(BF16)
            grad = dot_nn(dscores, keys) * (inverse * scale)
            out[rows, cols] = (grad + lq[rows, cols]).astype(BF16)


def memory_part(slots, tiles, q, gm, lq, units, heads, top, scale):
    tokens, width = q.shape
    groups = tokens // BLK * heads
    return pl.pallas_call(
        functools.partial(memory_kernel, units, heads, top, scale),
        out_shape=jax.ShapeDtypeStruct((tokens, width), BF16),
        in_specs=[SMEM, ANY, VMEM, VMEM, VMEM],
        out_specs=VMEM,
        scratch_shapes=[
            pltpu.VMEM((groups, top * BLK, DH), BF16),
            pltpu.VMEM((groups, top * BLK, DH), BF16),
            pltpu.SemaphoreType.DMA((2 * groups * top,)),
        ],
        cost_estimate=pl.CostEstimate(
            flops=6 * groups * BLK * top * BLK * DH, transcendentals=groups * BLK * top * BLK, bytes_accessed=5 << 20
        ),
        name="memory_part",
    )(slots, tiles, q, gm, lq)


def join_kernel(*refs):
    *parts, out = refs
    rows = parts[0].shape[0]
    for i, part in enumerate(parts):
        out[i * rows : (i + 1) * rows] = part[...]


def join(parts):
    rows, width = parts[0].shape
    return pl.pallas_call(
        join_kernel,
        out_shape=jax.ShapeDtypeStruct((rows * len(parts), width), parts[0].dtype),
        in_specs=[VMEM] * len(parts),
        out_specs=VMEM,
        name="join",
    )(*parts)


def head_kernel(order, go_a, go_b, w_a, w_b, out):
    part = dot_nn(
        jnp.concatenate([go_a[...], go_b[...]], axis=1), jnp.concatenate([w_a[...], w_b[...]], axis=0)
    )

    @pl.when(pl.program_id(0) == 0)
    def _():
        out[...] = part

    @pl.when(pl.program_id(0) > 0)
    def _():
        out[...] += part


def head_part(order, grad_out, w_a, w_b):
    tokens = grad_out.shape[0]
    rows, width = w_a.shape
    steps = rows // BLK
    return pl.pallas_call(
        head_kernel,
        grid_spec=pltpu.PrefetchScalarGridSpec(
            num_scalar_prefetch=1,
            grid=(steps,),
            in_specs=[
                pl.BlockSpec((tokens, BLK), lambda k, order: (0, order[0, k])),
                pl.BlockSpec((tokens, BLK), lambda k, order: (0, order[1, k])),
                pl.BlockSpec((BLK, width), lambda k, order: (k, 0)),
                pl.BlockSpec((BLK, width), lambda k, order: (k, 0)),
            ],
            out_specs=pl.BlockSpec((tokens, width), lambda k, order: (0, 0)),
        ),
        out_shape=jax.ShapeDtypeStruct((tokens, width), F32),
        cost_estimate=pl.CostEstimate(
            flops=4 * tokens * rows * width, transcendentals=0, bytes_accessed=9 << 20
        ),
        name="head_part",
    )(order, grad_out, grad_out, w_a, w_b)


def local_kernel(scale, window, start, gate, q, k, v, halo, hg, gm_out, lq_out, gk_out, gv_out, back_out):
    head = pl.program_id(0)
    share = gate[head]
    blocks = q.shape[0] // BLK
    key_blocks = [halo[0, :BLK], halo[0, BLK:]] + [k[i * BLK : (i + 1) * BLK] for i in range(blocks)]
    val_blocks = [halo[1, :BLK], halo[1, BLK:]] + [v[i * BLK : (i + 1) * BLK] for i in range(blocks)]
    key_sums = [None] * (blocks + 2)
    val_sums = [None] * (blocks + 2)
    row = lax.broadcasted_iota(jnp.int32, (BLK, 3 * BLK), 0)
    col = lax.broadcasted_iota(jnp.int32, (BLK, 3 * BLK), 1) - 2 * BLK
    for b in range(blocks):
        rows = slice(b * BLK, (b + 1) * BLK)
        grad = hg[rows, :]
        gm_out[rows, :] = (share * grad).astype(BF16)
        gl = ((1.0 - share) * grad).astype(BF16)
        qb = q[rows, :]
        keys = jnp.concatenate(key_blocks[b : b + 3], axis=0)
        vals = jnp.concatenate(val_blocks[b : b + 3], axis=0)
        allowed = (col <= row) & (col > row - window[b]) & (col + b * BLK >= -start[0])
        scores = jnp.where(allowed, dot_nt(qb, keys) * scale, -1e30)
        expo = jnp.exp(scores - jnp.max(scores, axis=-1, keepdims=True))
        probs = expo * (1.0 / jnp.sum(expo, axis=-1, keepdims=True))
        dprobs = dot_nt(gl, vals)
        delta = jnp.sum(probs * dprobs, axis=-1, keepdims=True)
        dscores = (probs * (dprobs - delta)).astype(BF16)
        probs16 = probs.astype(BF16)
        lq_out[rows, :] = dot_nn(dscores, keys) * scale
        key_grad = dot_tn(dscores, qb)
        val_grad = dot_tn(probs16, gl)
        for j in range(3):
            part = slice(j * BLK, (j + 1) * BLK)
            for sums, grads in ((key_sums, key_grad), (val_sums, val_grad)):
                sums[b + j] = grads[part] if sums[b + j] is None else sums[b + j] + grads[part]
    for i in range(2):
        back_out[0, i * BLK : (i + 1) * BLK, :] = (key_sums[i] * scale).astype(BF16)
        back_out[1, i * BLK : (i + 1) * BLK, :] = val_sums[i].astype(BF16)
    for i in range(blocks):
        gk_out[i * BLK : (i + 1) * BLK, :] = key_sums[i + 2] * scale
        gv_out[i * BLK : (i + 1) * BLK, :] = val_sums[i + 2]


def local_part(window, start, gate, q, k, v, halo, hg, scale):
    tokens, width = q.shape
    heads = width // DH
    column = pl.BlockSpec((tokens, DH), lambda h: (0, h))
    pair = pl.BlockSpec((2, 2 * BLK, DH), lambda h: (0, 0, h))
    return pl.pallas_call(
        functools.partial(local_kernel, scale),
        grid=(heads,),
        out_shape=(
            jax.ShapeDtypeStruct((tokens, width), BF16),
            jax.ShapeDtypeStruct((tokens, width), F32),
            jax.ShapeDtypeStruct((tokens, width), F32),
            jax.ShapeDtypeStruct((tokens, width), F32),
            jax.ShapeDtypeStruct((2, 2 * BLK, width), BF16),
        ),
        in_specs=[SMEM, SMEM, SMEM, column, column, column, pair, column],
        out_specs=(column, column, column, column, pair),
        cost_estimate=pl.CostEstimate(
            flops=10 * tokens * 3 * BLK * width, transcendentals=tokens * 3 * BLK * heads, bytes_accessed=6 << 20
        ),
        name="local_part",
    )(window, start, gate, q, k, v, halo, hg)


def place_of(x, y, core):
    return (x % 4) * 8 + (y % 4) * 2 + core


def torus(shift, phase):
    pairs = []
    for x in range(4):
        for y in range(4):
            for core in range(2):
                dx, dy = (shift, 0) if core == phase else (0, shift)
                pairs.append((place_of(x, y, core), place_of(x + dx, y + dy, core)))
    return pairs


def arrival(me):
    x, y, core = me >> 3, (me >> 1) & 3, me & 1
    step = jnp.arange(16, dtype=jnp.int32)
    first, second = step & 3, step >> 2
    south = place_of(x - first, y - second, 0)
    north = place_of(x - second, y - first, 1)
    return jnp.where(core == 0, jnp.stack([south, north]), jnp.stack([north, south]))


def body(
    queries,
    local_keys,
    local_values,
    memory_keys,
    memory_values,
    grad_out,
    out_weight,
    gate_logits,
    tile_ids,
    window,
):
    _, heads, top = tile_ids.shape
    members = lax.axis_size("mem")
    me = lax.axis_index("mem")
    core = (me & 1).reshape(1)
    scale = 1.0 / math.sqrt(DH)
    tokens = queries.shape[0]

    request, slots = requests(tile_ids, members)
    codes = lax.all_to_all(request, "mem", split_axis=0, concat_axis=0, tiled=True)

    partner = [(i, i ^ 1) for i in range(members)]
    peer_keys = lax.ppermute(memory_keys, "mem", partner)
    peer_vals = lax.ppermute(memory_values, "mem", partner)
    rows = [out_weight] + [lax.ppermute(out_weight, "mem", torus(shift, 0)) for shift in (1, 2, 3)]
    sources = (codes, core, memory_keys, memory_values, peer_keys, peer_vals)
    sent = gather_tiles(*sources, 0, UNITS).reshape(members, UNITS, BLK, DH)
    band = join(rows)
    bands = [band] + [lax.ppermute(band, "mem", torus(shift, 1)) for shift in (1, 2, 3)]
    halo = jnp.stack([local_keys[tokens - 2 * BLK :], local_values[tokens - 2 * BLK :]])
    halo = lax.ppermute(halo, "mem", [(i, i + 1) for i in range(members - 1)])
    tiles = lax.all_to_all(sent, "mem", split_axis=0, concat_axis=0, tiled=True)

    w_own = join(bands)
    w_peer = lax.ppermute(w_own, "mem", partner)
    head_grad = head_part(arrival(me), grad_out, w_own, w_peer)
    gate = jax.nn.sigmoid(gate_logits)
    start = (me * tokens).reshape(1)
    gm, lq, gk, gv, back = local_part(
        window, start, gate, queries, local_keys, local_values, halo, head_grad, scale
    )
    back = lax.ppermute(back, "mem", [(i + 1, i) for i in range(members - 1)])
    grad_keys, grad_values = closing(gk, gv, back)

    def usual():
        flat = tiles.reshape(members * UNITS, BLK, DH)
        return memory_part(slots, flat, queries, gm, lq, UNITS, heads, top, scale)

    def with_sixth():
        sixth = gather_tiles(*sources, UNITS, 1).reshape(members, 1, BLK, DH)
        sixth = lax.all_to_all(sixth, "mem", split_axis=0, concat_axis=0, tiled=True)
        flat = jnp.concatenate([tiles, sixth], axis=1).reshape(members * (UNITS + 1), BLK, DH)
        return memory_part(slots, flat, queries, gm, lq, UNITS + 1, heads, top, scale)

    grad_queries = lax.cond(jnp.max(codes[:, 0, FLAG]) > 0, with_sixth, usual)
    return grad_queries, grad_keys, grad_values


def solution(mesh):
    in_specs = (
        P("mem", "mp"),
        P("mem", "mp"),
        P("mem", "mp"),
        P("mem", "mp"),
        P("mem", "mp"),
        P("mem", None),
        P("mem", "mp"),
        P("mp"),
        P("mem", "mp", None),
        P("mem"),
    )
    out_specs = (P("mem", "mp"), P("mem", "mp"), P("mem", "mp"))

    return jax.shard_map(body, mesh=mesh, in_specs=in_specs, out_specs=out_specs, check_vma=False)
```

```python
import functools
import math

import jax
import jax.numpy as jnp
from jax import lax
from jax.experimental import pallas as pl
from jax.experimental.pallas import tpu as pltpu
from jax.sharding import PartitionSpec as P


BLK = 128
DH = 128
UNITS = 5
LANES = 128
FLAG = 8
LOG2E = 1.4426950408889634
BF16 = jnp.bfloat16
F32 = jnp.float32
ANY = pl.BlockSpec(memory_space=pl.ANY)
HBM = pl.BlockSpec(memory_space=pltpu.HBM)
SMEM = pl.BlockSpec(memory_space=pltpu.SMEM)
VMEM = pl.BlockSpec(memory_space=pltpu.VMEM)


def dot_nt(a, b):
    return lax.dot_general(a, b, (((1,), (1,)), ((), ())), preferred_element_type=F32)


def dot_nn(a, b):
    return lax.dot_general(a, b, (((1,), (0,)), ((), ())), preferred_element_type=F32)


def dot_tn(a, b):
    return lax.dot_general(a, b, (((0,), (0,)), ((), ())), preferred_element_type=F32)


def request_kernel(ids, request, slots, filled, third):
    blocks, heads, top = ids.shape
    members = request.shape[0]

    def clear(chip, carry):
        filled[2 * chip] = 0
        filled[2 * chip + 1] = 0
        third[chip] = 2
        for lane in range(UNITS + 1):
            request[2 * chip, 0, lane] = -1
            request[2 * chip + 1, 0, lane] = -1
        return carry

    def enter(group, over):
        block, head = group // heads, group % heads
        for t in range(top):
            tile = ids[block, head, t]
            owner, chip = tile >> 4, tile >> 5
            have = filled[owner]
            filled[owner] = have + 1
            spare = third[chip]
            third[chip] = jnp.where(have == 2, UNITS, spare)
            place = jnp.where(have == 2, spare, jnp.where((owner & 1) == 0, have, UNITS - 1 - have))
            code = (tile & 31) * heads + head
            request[2 * chip, 0, place] = code
            request[2 * chip + 1, 0, place] = code
            slots[group * top + t] = chip * 8 + place
            over = jnp.maximum(over, place)
        return over

    def flag(member, over):
        request[member, 0, FLAG] = (over >= UNITS).astype(jnp.int32)
        return over

    lax.fori_loop(0, members // 2, clear, 0)
    over = lax.fori_loop(0, blocks * heads, enter, jnp.int32(0))
    lax.fori_loop(0, members, flag, over)


def requests(ids, members):
    return pl.pallas_call(
        request_kernel,
        out_shape=(
            jax.ShapeDtypeStruct((members, 1, LANES), jnp.int32),
            jax.ShapeDtypeStruct((ids.size,), jnp.int32),
        ),
        in_specs=[SMEM],
        out_specs=(SMEM, SMEM),
        scratch_shapes=[pltpu.SMEM((members,), jnp.int32), pltpu.SMEM((members // 2,), jnp.int32)],
        name="requests",
    )(ids)


def gather_kernel(first, units, codes, core, keys, vals, peer_keys, peer_vals, out, stage, taken, given):
    members = codes.shape[0]

    def fetch_all(sources):
        def member(dest, carry):
            for unit in range(units):
                code = codes[dest, 0, first + unit]
                row = pl.multiple_of(((code >> 2) & 15) * BLK, BLK)
                col = pl.multiple_of((code & 3) * DH, DH)

                def fetch(source):
                    tile = source.at[pl.ds(row, BLK), pl.ds(col, DH)]
                    pltpu.make_async_copy(tile, stage.at[dest, unit], taken.at[dest, unit]).start()

                if first + unit in (2, UNITS):
                    for side in range(2):
                        pl.when((code >> 6) == side)(functools.partial(fetch, sources[side]))
                else:
                    pl.when(code >= 0)(functools.partial(fetch, sources[(first + unit) // 3]))
            return carry

        lax.fori_loop(0, members, member, 0)

    @pl.when(core[0] == 0)
    def _():
        fetch_all((keys, peer_keys))

    @pl.when(core[0] == 1)
    def _():
        fetch_all((peer_vals, vals))

    def give(dest):
        return pltpu.make_async_copy(stage.at[dest], out.at[dest], given.at[dest])

    def pass_on(dest, carry):
        for unit in range(units):

            @pl.when(codes[dest, 0, first + unit] >= 0)
            def _():
                tile = stage.at[dest, unit]
                pltpu.make_async_copy(tile, tile, taken.at[dest, unit]).wait()

        give(dest).start()
        return carry

    def settle(dest, carry):
        give(dest).wait()
        return carry

    lax.fori_loop(0, members, pass_on, 0)
    lax.fori_loop(0, members, settle, 0)


def gather_tiles(codes, core, keys, vals, peer_keys, peer_vals, first, units):
    members = codes.shape[0]
    return pl.pallas_call(
        functools.partial(gather_kernel, first, units),
        out_shape=jax.ShapeDtypeStruct((members, units, BLK, DH), BF16),
        in_specs=[SMEM, SMEM, HBM, HBM, HBM, HBM],
        out_specs=HBM,
        scratch_shapes=[
            pltpu.VMEM((members, units, BLK, DH), BF16),
            pltpu.SemaphoreType.DMA((members, units)),
            pltpu.SemaphoreType.DMA((members,)),
        ],
        name="gather_tiles",
    )(codes, core, keys, vals, peer_keys, peer_vals)


def closing_kernel(gk, gv, back, gk_out, gv_out):
    rest = gk.shape[0] - 2 * BLK
    for i, own, out in ((0, gk, gk_out), (1, gv, gv_out)):
        out[:rest] = own[:rest].astype(BF16)
        out[rest:] = (own[rest:] + back[i].astype(F32)).astype(BF16)


def closing(gk, gv, back):
    return pl.pallas_call(
        closing_kernel,
        out_shape=(jax.ShapeDtypeStruct(gk.shape, BF16), jax.ShapeDtypeStruct(gv.shape, BF16)),
        in_specs=[VMEM, VMEM, VMEM],
        out_specs=(VMEM, VMEM),
        name="closing",
    )(gk, gv, back)


def memory_kernel(
    units, heads, top, scale, slots, tiles, q, gm, lq, out, kbuf, vbuf, qbuf, gbuf, lbuf, obuf, sems, ends
):
    blocks = q.shape[0] // BLK
    loads = [
        pltpu.make_async_copy(source, target, ends.at[i])
        for i, (source, target) in enumerate(((q, qbuf), (gm, gbuf), (lq, lbuf)))
    ]

    def copies(r):
        slot = slots[r]
        base = (slot >> 3) * 2 * units + (slot & 7)
        rows = pl.ds(pl.multiple_of((r % top) * BLK, BLK), BLK)
        return (
            pltpu.make_async_copy(tiles.at[base], kbuf.at[r // top, rows], sems.at[2 * r]),
            pltpu.make_async_copy(tiles.at[base + units], vbuf.at[r // top, rows], sems.at[2 * r + 1]),
        )

    def issue(r, carry):
        for one in copies(r):
            one.start()
        return carry

    def store(b):
        rows = pl.ds(b * BLK, BLK)
        return pltpu.make_async_copy(obuf.at[rows], out.at[rows], ends.at[3 + b])

    first = heads * top
    loads[0].start()
    lax.fori_loop(0, first, issue, 0)
    loads[1].start()
    loads[2].start()
    lax.fori_loop(first, blocks * first, issue, 0)
    for load in loads:
        load.wait()
    for b in range(blocks):
        rows = slice(b * BLK, (b + 1) * BLK)
        for r in range(b * heads * top, (b + 1) * heads * top):
            for one in copies(r):
                one.wait()
        span = range(heads)
        cols = [slice(h * DH, (h + 1) * DH) for h in span]
        keys = [kbuf[b * heads + h] for h in span]
        scores = [dot_nt(qbuf[rows, cols[h]], keys[h]) for h in span]
        dprobs = [dot_nt(gbuf[rows, cols[h]], vbuf[b * heads + h]) for h in span]
        expo = [jnp.exp2((x - jnp.max(x, axis=-1, keepdims=True)) * (scale * LOG2E)) for x in scores]
        inverse = [1.0 / jnp.sum(x, axis=-1, keepdims=True) for x in expo]
        delta = [jnp.sum(expo[h] * dprobs[h], axis=-1, keepdims=True) * inverse[h] for h in span]
        dscores = [(expo[h] * (dprobs[h] - delta[h])).astype(BF16) for h in span]
        for h in span:
            grad = dot_nn(dscores[h], keys[h]) * (inverse[h] * scale)
            obuf[rows, cols[h]] = (grad + lbuf[rows, cols[h]]).astype(BF16)
        store(b).start()
    for b in range(blocks):
        store(b).wait()


def memory_part(slots, tiles, q, gm, lq, units, heads, top, scale):
    tokens, width = q.shape
    blocks = tokens // BLK
    groups = blocks * heads
    return pl.pallas_call(
        functools.partial(memory_kernel, units, heads, top, scale),
        out_shape=jax.ShapeDtypeStruct((tokens, width), BF16),
        in_specs=[SMEM, ANY, ANY, ANY, ANY],
        out_specs=ANY,
        scratch_shapes=[
            pltpu.VMEM((groups, top * BLK, DH), BF16),
            pltpu.VMEM((groups, top * BLK, DH), BF16),
            pltpu.VMEM((tokens, width), BF16),
            pltpu.VMEM((tokens, width), BF16),
            pltpu.VMEM((tokens, width), F32),
            pltpu.VMEM((tokens, width), BF16),
            pltpu.SemaphoreType.DMA((2 * groups * top,)),
            pltpu.SemaphoreType.DMA((3 + blocks,)),
        ],
        cost_estimate=pl.CostEstimate(
            flops=6 * groups * BLK * top * BLK * DH, transcendentals=groups * BLK * top * BLK, bytes_accessed=5 << 20
        ),
        name="memory_part",
    )(slots, tiles, q, gm, lq)


def join_kernel(pieces, *refs):
    outs = 1 + max(piece[0] for piece in pieces)
    sources, targets, stages, (taken, given) = (
        refs[: -2 * outs - 2],
        refs[-2 * outs - 2 : -outs - 2],
        refs[-outs - 2 : -2],
        refs[-2:],
    )
    count = [0] * outs
    steps = []
    for i, (out, source, row) in enumerate(pieces):
        rows = stages[out].shape[0] // sum(piece[0] == out for piece in pieces)
        here = pl.ds(count[out] * rows, rows)
        count[out] += 1
        steps.append(
            (
                pltpu.make_async_copy(sources[source].at[pl.ds(row, rows)], stages[out].at[here], taken.at[i]),
                pltpu.make_async_copy(stages[out].at[here], targets[out].at[here], given.at[i]),
            )
        )
    for take, _ in steps:
        take.start()
    for take, give in steps:
        take.wait()
        give.start()
    for _, give in steps:
        give.wait()


def join(pieces, sources, rows):
    width = sources[0].shape[1]
    shapes = [(n, width) for n in rows]
    return pl.pallas_call(
        functools.partial(join_kernel, tuple(pieces)),
        out_shape=tuple(jax.ShapeDtypeStruct(shape, BF16) for shape in shapes),
        in_specs=[HBM] * len(sources),
        out_specs=(HBM,) * len(rows),
        scratch_shapes=[pltpu.VMEM(shape, BF16) for shape in shapes]
        + [pltpu.SemaphoreType.DMA((len(pieces),)), pltpu.SemaphoreType.DMA((len(pieces),))],
        name="join",
    )(*sources)


def head_kernel(order, go_a, go_b, w_a, w_b, out):
    part = dot_nn(
        jnp.concatenate([go_a[...], go_b[...]], axis=1), jnp.concatenate([w_a[...], w_b[...]], axis=0)
    )

    @pl.when(pl.program_id(0) == 0)
    def _():
        out[...] = part

    @pl.when(pl.program_id(0) > 0)
    def _():
        out[...] += part


def head_part(order, grad_out, w_a, w_b):
    tokens = grad_out.shape[0]
    rows, width = w_a.shape
    steps = rows // BLK
    return pl.pallas_call(
        head_kernel,
        grid_spec=pltpu.PrefetchScalarGridSpec(
            num_scalar_prefetch=1,
            grid=(steps,),
            in_specs=[
                pl.BlockSpec((tokens, BLK), lambda k, order: (0, order[0, k])),
                pl.BlockSpec((tokens, BLK), lambda k, order: (0, order[1, k])),
                pl.BlockSpec((BLK, width), lambda k, order: (k, 0)),
                pl.BlockSpec((BLK, width), lambda k, order: (k, 0)),
            ],
            out_specs=pl.BlockSpec((tokens, width), lambda k, order: (0, 0)),
        ),
        out_shape=jax.ShapeDtypeStruct((tokens, width), F32),
        cost_estimate=pl.CostEstimate(
            flops=4 * tokens * rows * width, transcendentals=0, bytes_accessed=9 << 20
        ),
        name="head_part",
    )(order, grad_out, grad_out, w_a, w_b)


def local_kernel(scale, window, start, gate, q, k, v, hk, hv, hg, gm_out, lq_out, gk_out, gv_out, back_out):
    head = pl.program_id(0)
    share = gate[head]
    blocks = q.shape[0] // BLK
    tail = q.shape[0] - 2 * BLK
    key_blocks = [hk[tail : tail + BLK], hk[tail + BLK :]] + [k[i * BLK : (i + 1) * BLK] for i in range(blocks)]
    val_blocks = [hv[tail : tail + BLK], hv[tail + BLK :]] + [v[i * BLK : (i + 1) * BLK] for i in range(blocks)]
    key_sums = [None] * (blocks + 2)
    val_sums = [None] * (blocks + 2)
    row = lax.broadcasted_iota(jnp.int32, (BLK, 3 * BLK), 0)
    col = lax.broadcasted_iota(jnp.int32, (BLK, 3 * BLK), 1) - 2 * BLK
    for b in range(blocks):
        rows = slice(b * BLK, (b + 1) * BLK)
        grad = hg[rows, :]
        gm_out[rows, :] = (share * grad).astype(BF16)
        gl = ((1.0 - share) * grad).astype(BF16)
        qb = q[rows, :]
        keys = jnp.concatenate(key_blocks[b : b + 3], axis=0)
        vals = jnp.concatenate(val_blocks[b : b + 3], axis=0)
        allowed = (col <= row) & (col > row - window[b]) & (col + b * BLK >= -start[0])
        scores = jnp.where(allowed, dot_nt(qb, keys) * scale, -1e30)
        expo = jnp.exp(scores - jnp.max(scores, axis=-1, keepdims=True))
        probs = expo * (1.0 / jnp.sum(expo, axis=-1, keepdims=True))
        dprobs = dot_nt(gl, vals)
        delta = jnp.sum(probs * dprobs, axis=-1, keepdims=True)
        dscores = (probs * (dprobs - delta)).astype(BF16)
        probs16 = probs.astype(BF16)
        lq_out[rows, :] = dot_nn(dscores, keys) * scale
        key_grad = dot_tn(dscores, qb)
        val_grad = dot_tn(probs16, gl)
        for j in range(3):
            part = slice(j * BLK, (j + 1) * BLK)
            for sums, grads in ((key_sums, key_grad), (val_sums, val_grad)):
                sums[b + j] = grads[part] if sums[b + j] is None else sums[b + j] + grads[part]
    for i in range(2):
        back_out[0, i * BLK : (i + 1) * BLK, :] = (key_sums[i] * scale).astype(BF16)
        back_out[1, i * BLK : (i + 1) * BLK, :] = val_sums[i].astype(BF16)
    for i in range(blocks):
        gk_out[i * BLK : (i + 1) * BLK, :] = key_sums[i + 2] * scale
        gv_out[i * BLK : (i + 1) * BLK, :] = val_sums[i + 2]


def local_part(window, start, gate, q, k, v, hk, hv, hg, scale):
    tokens, width = q.shape
    heads = width // DH
    column = pl.BlockSpec((tokens, DH), lambda h: (0, h))
    pair = pl.BlockSpec((2, 2 * BLK, DH), lambda h: (0, 0, h))
    return pl.pallas_call(
        functools.partial(local_kernel, scale),
        grid=(heads,),
        out_shape=(
            jax.ShapeDtypeStruct((tokens, width), BF16),
            jax.ShapeDtypeStruct((tokens, width), F32),
            jax.ShapeDtypeStruct((tokens, width), F32),
            jax.ShapeDtypeStruct((tokens, width), F32),
            jax.ShapeDtypeStruct((2, 2 * BLK, width), BF16),
        ),
        in_specs=[SMEM, SMEM, SMEM, column, column, column, column, column, column],
        out_specs=(column, column, column, column, pair),
        cost_estimate=pl.CostEstimate(
            flops=10 * tokens * 3 * BLK * width, transcendentals=tokens * 3 * BLK * heads, bytes_accessed=6 << 20
        ),
        name="local_part",
    )(window, start, gate, q, k, v, hk, hv, hg)


def place_of(x, y, core):
    return (x % 4) * 8 + (y % 4) * 2 + core


def torus(shift, phase):
    pairs = []
    for x in range(4):
        for y in range(4):
            for core in range(2):
                dx, dy = (shift, 0) if core == phase else (0, shift)
                pairs.append((place_of(x, y, core), place_of(x + dx, y + dy, core)))
    return pairs


def arrival(me):
    x, y, core = me >> 3, (me >> 1) & 3, me & 1
    step = jnp.arange(16, dtype=jnp.int32)
    first, second = step & 3, step >> 2
    south = place_of(x - first, y - second, 0)
    north = place_of(x - second, y - first, 1)
    return jnp.where(core == 0, jnp.stack([south, north]), jnp.stack([north, south]))


def body(
    queries,
    local_keys,
    local_values,
    memory_keys,
    memory_values,
    grad_out,
    out_weight,
    gate_logits,
    tile_ids,
    window,
):
    _, heads, top = tile_ids.shape
    members = lax.axis_size("mem")
    me = lax.axis_index("mem")
    core = (me & 1).reshape(1)
    scale = 1.0 / math.sqrt(DH)
    tokens = queries.shape[0]

    onward = [(i, (i + 1) % members) for i in range(members)]
    halo_keys = lax.ppermute(local_keys, "mem", onward)
    halo_values = lax.ppermute(local_values, "mem", onward)

    request, slots = requests(tile_ids, members)
    codes = lax.all_to_all(request, "mem", split_axis=0, concat_axis=0, tiled=True)

    partner = [(i, i ^ 1) for i in range(members)]
    peer_keys = lax.ppermute(memory_keys, "mem", partner)
    peer_vals = lax.ppermute(memory_values, "mem", partner)
    rows = [out_weight] + [lax.ppermute(out_weight, "mem", torus(shift, 0)) for shift in (1, 2, 3)]
    sources = (codes, core, memory_keys, memory_values, peer_keys, peer_vals)
    sent = gather_tiles(*sources, 0, UNITS)
    (band,) = join([(0, i, 0) for i in range(4)], rows, (4 * out_weight.shape[0],))
    bands = [band] + [lax.ppermute(band, "mem", torus(shift, 1)) for shift in (1, 2, 3)]
    tiles = lax.all_to_all(sent, "mem", split_axis=0, concat_axis=0, tiled=True)

    (w_own,) = join([(0, i, 0) for i in range(4)], bands, (4 * band.shape[0],))
    w_peer = lax.ppermute(w_own, "mem", partner)
    head_grad = head_part(arrival(me), grad_out, w_own, w_peer)
    gate = jax.nn.sigmoid(gate_logits)
    start = (me * tokens).reshape(1)
    gm, lq, gk, gv, back = local_part(
        window, start, gate, queries, local_keys, local_values, halo_keys, halo_values, head_grad, scale
    )
    back = lax.ppermute(back, "mem", [(i + 1, i) for i in range(members - 1)])
    grad_keys, grad_values = closing(gk, gv, back)

    def usual():
        flat = tiles.reshape(members * UNITS, BLK, DH)
        return memory_part(slots, flat, queries, gm, lq, UNITS, heads, top, scale)

    def with_sixth():
        sixth = gather_tiles(*sources, UNITS, 1)
        sixth = lax.all_to_all(sixth, "mem", split_axis=0, concat_axis=0, tiled=True)
        flat = jnp.concatenate([tiles, sixth], axis=1).reshape(members * (UNITS + 1), BLK, DH)
        return memory_part(slots, flat, queries, gm, lq, UNITS + 1, heads, top, scale)

    grad_queries = lax.cond(jnp.max(codes[:, 0, FLAG]) > 0, with_sixth, usual)
    return grad_queries, grad_keys, grad_values


def solution(mesh):
    in_specs = (
        P("mem", "mp"),
        P("mem", "mp"),
        P("mem", "mp"),
        P("mem", "mp"),
        P("mem", "mp"),
        P("mem", None),
        P("mem", "mp"),
        P("mp"),
        P("mem", "mp", None),
        P("mem"),
    )
    out_specs = (P("mem", "mp"), P("mem", "mp"), P("mem", "mp"))

    return jax.shard_map(body, mesh=mesh, in_specs=in_specs, out_specs=out_specs, check_vma=False)
```

```python
import functools
import math

import jax
import jax.numpy as jnp
from jax import lax
from jax.experimental import pallas as pl
from jax.experimental.pallas import tpu as pltpu
from jax.sharding import PartitionSpec as P


BLK = 128
DH = 128
UNITS = 5
LANES = 128
FLAG = 8
LOG2E = 1.4426950408889634
BF16 = jnp.bfloat16
F32 = jnp.float32
ANY = pl.BlockSpec(memory_space=pl.ANY)
HBM = pl.BlockSpec(memory_space=pltpu.HBM)
SMEM = pl.BlockSpec(memory_space=pltpu.SMEM)
VMEM = pl.BlockSpec(memory_space=pltpu.VMEM)


def dot_nt(a, b):
    return lax.dot_general(a, b, (((1,), (1,)), ((), ())), preferred_element_type=F32)


def dot_nn(a, b):
    return lax.dot_general(a, b, (((1,), (0,)), ((), ())), preferred_element_type=F32)


def dot_tn(a, b):
    return lax.dot_general(a, b, (((0,), (0,)), ((), ())), preferred_element_type=F32)


def request_kernel(ids, request, slots, filled, third):
    blocks, heads, top = ids.shape
    members = request.shape[0]

    def clear(chip, carry):
        filled[2 * chip] = 0
        filled[2 * chip + 1] = 0
        third[chip] = 2
        for lane in range(UNITS + 1):
            request[2 * chip, 0, lane] = -1
            request[2 * chip + 1, 0, lane] = -1
        return carry

    def enter(group, over):
        block, head = group // heads, group % heads
        for t in range(top):
            tile = ids[block, head, t]
            owner, chip = tile >> 4, tile >> 5
            have = filled[owner]
            filled[owner] = have + 1
            spare = third[chip]
            third[chip] = jnp.where(have == 2, UNITS, spare)
            place = jnp.where(have == 2, spare, jnp.where((owner & 1) == 0, have, UNITS - 1 - have))
            code = (tile & 31) * heads + head
            request[2 * chip, 0, place] = code
            request[2 * chip + 1, 0, place] = code
            slots[group * top + t] = chip * 8 + place
            over = jnp.maximum(over, place)
        return over

    def flag(member, over):
        request[member, 0, FLAG] = (over >= UNITS).astype(jnp.int32)
        return over

    lax.fori_loop(0, members // 2, clear, 0)
    over = lax.fori_loop(0, blocks * heads, enter, jnp.int32(0))
    lax.fori_loop(0, members, flag, over)


def requests(ids, members):
    return pl.pallas_call(
        request_kernel,
        out_shape=(
            jax.ShapeDtypeStruct((members, 1, LANES), jnp.int32),
            jax.ShapeDtypeStruct((ids.size,), jnp.int32),
        ),
        in_specs=[SMEM],
        out_specs=(SMEM, SMEM),
        scratch_shapes=[pltpu.SMEM((members,), jnp.int32), pltpu.SMEM((members // 2,), jnp.int32)],
        name="requests",
    )(ids)


def gather_kernel(first, units, codes, core, keys, vals, peer_keys, peer_vals, out, stage, taken, given):
    members = codes.shape[0]

    def fetch_all(sources):
        def member(dest, carry):
            for unit in range(units):
                code = codes[dest, 0, first + unit]
                row = pl.multiple_of(((code >> 2) & 15) * BLK, BLK)
                col = pl.multiple_of((code & 3) * DH, DH)

                def fetch(source):
                    tile = source.at[pl.ds(row, BLK), pl.ds(col, DH)]
                    pltpu.make_async_copy(tile, stage.at[dest, unit], taken.at[dest, unit]).start()

                if first + unit in (2, UNITS):
                    for side in range(2):
                        pl.when((code >> 6) == side)(functools.partial(fetch, sources[side]))
                else:
                    pl.when(code >= 0)(functools.partial(fetch, sources[(first + unit) // 3]))
            return carry

        lax.fori_loop(0, members, member, 0)

    @pl.when(core[0] == 0)
    def _():
        fetch_all((keys, peer_keys))

    @pl.when(core[0] == 1)
    def _():
        fetch_all((peer_vals, vals))

    def give(dest):
        return pltpu.make_async_copy(stage.at[dest], out.at[dest], given.at[dest])

    def pass_on(dest, carry):
        for unit in range(units):

            @pl.when(codes[dest, 0, first + unit] >= 0)
            def _():
                tile = stage.at[dest, unit]
                pltpu.make_async_copy(tile, tile, taken.at[dest, unit]).wait()

        give(dest).start()
        return carry

    def settle(dest, carry):
        give(dest).wait()
        return carry

    lax.fori_loop(0, members, pass_on, 0)
    lax.fori_loop(0, members, settle, 0)


def gather_tiles(codes, core, keys, vals, peer_keys, peer_vals, first, units):
    members = codes.shape[0]
    return pl.pallas_call(
        functools.partial(gather_kernel, first, units),
        out_shape=jax.ShapeDtypeStruct((members, units, BLK, DH), BF16),
        in_specs=[SMEM, SMEM, HBM, HBM, HBM, HBM],
        out_specs=HBM,
        scratch_shapes=[
            pltpu.VMEM((members, units, BLK, DH), BF16),
            pltpu.SemaphoreType.DMA((members, units)),
            pltpu.SemaphoreType.DMA((members,)),
        ],
        name="gather_tiles",
    )(codes, core, keys, vals, peer_keys, peer_vals)


def memory_kernel(
    units,
    heads,
    top,
    scale,
    slots,
    tiles,
    q,
    gm,
    lq,
    own,
    back,
    out,
    gk_out,
    gv_out,
    kbuf,
    vbuf,
    qbuf,
    gbuf,
    lbuf,
    obuf,
    own_buf,
    back_buf,
    sum_buf,
    sems,
    ends,
    closes,
):
    rest = q.shape[0] - 2 * BLK
    own_load = pltpu.make_async_copy(own, own_buf, closes.at[0])
    back_load = pltpu.make_async_copy(back, back_buf, closes.at[1])
    closing = [
        pltpu.make_async_copy(sum_buf.at[i], target, closes.at[2 + i]) for i, target in ((0, gk_out), (1, gv_out))
    ]
    blocks = q.shape[0] // BLK
    loads = [
        pltpu.make_async_copy(source, target, ends.at[i])
        for i, (source, target) in enumerate(((q, qbuf), (gm, gbuf), (lq, lbuf)))
    ]

    def copies(r):
        slot = slots[r]
        base = (slot >> 3) * 2 * units + (slot & 7)
        rows = pl.ds(pl.multiple_of((r % top) * BLK, BLK), BLK)
        return (
            pltpu.make_async_copy(tiles.at[base], kbuf.at[r // top, rows], sems.at[2 * r]),
            pltpu.make_async_copy(tiles.at[base + units], vbuf.at[r // top, rows], sems.at[2 * r + 1]),
        )

    def issue(r, carry):
        for one in copies(r):
            one.start()
        return carry

    def store(b):
        rows = pl.ds(b * BLK, BLK)
        return pltpu.make_async_copy(obuf.at[rows], out.at[rows], ends.at[3 + b])

    first = heads * top
    loads[0].start()
    lax.fori_loop(0, first, issue, 0)
    loads[1].start()
    loads[2].start()
    lax.fori_loop(first, blocks * first, issue, 0)
    own_load.start()
    back_load.start()
    for load in loads:
        load.wait()
    for b in range(blocks):
        rows = slice(b * BLK, (b + 1) * BLK)
        for r in range(b * heads * top, (b + 1) * heads * top):
            for one in copies(r):
                one.wait()
        span = range(heads)
        cols = [slice(h * DH, (h + 1) * DH) for h in span]
        keys = [kbuf[b * heads + h] for h in span]
        scores = [dot_nt(qbuf[rows, cols[h]], keys[h]) for h in span]
        dprobs = [dot_nt(gbuf[rows, cols[h]], vbuf[b * heads + h]) for h in span]
        expo = [jnp.exp2((x - jnp.max(x, axis=-1, keepdims=True)) * (scale * LOG2E)) for x in scores]
        inverse = [1.0 / jnp.sum(x, axis=-1, keepdims=True) for x in expo]
        delta = [jnp.sum(expo[h] * dprobs[h], axis=-1, keepdims=True) * inverse[h] for h in span]
        dscores = [(expo[h] * (dprobs[h] - delta[h])).astype(BF16) for h in span]
        for h in span:
            grad = dot_nn(dscores[h], keys[h]) * (inverse[h] * scale)
            obuf[rows, cols[h]] = (grad + lbuf[rows, cols[h]]).astype(BF16)
        store(b).start()
        if b == 1:
            own_load.wait()
            back_load.wait()
            for i in range(2):
                sum_buf[i, :rest] = own_buf[i, :rest].astype(BF16)
                sum_buf[i, rest:] = (own_buf[i, rest:] + back_buf[i].astype(F32)).astype(BF16)
                closing[i].start()
    for b in range(blocks):
        store(b).wait()
    for one in closing:
        one.wait()


def memory_part(slots, tiles, q, gm, lq, own, back, units, heads, top, scale):
    tokens, width = q.shape
    blocks = tokens // BLK
    groups = blocks * heads
    return pl.pallas_call(
        functools.partial(memory_kernel, units, heads, top, scale),
        out_shape=(jax.ShapeDtypeStruct((tokens, width), BF16),) * 3,
        in_specs=[SMEM, ANY, ANY, ANY, ANY, ANY, ANY],
        out_specs=(ANY, ANY, ANY),
        scratch_shapes=[
            pltpu.VMEM((groups, top * BLK, DH), BF16),
            pltpu.VMEM((groups, top * BLK, DH), BF16),
            pltpu.VMEM((tokens, width), BF16),
            pltpu.VMEM((tokens, width), BF16),
            pltpu.VMEM((tokens, width), F32),
            pltpu.VMEM((tokens, width), BF16),
            pltpu.VMEM((2, tokens, width), F32),
            pltpu.VMEM((2, 2 * BLK, width), BF16),
            pltpu.VMEM((2, tokens, width), BF16),
            pltpu.SemaphoreType.DMA((2 * groups * top,)),
            pltpu.SemaphoreType.DMA((3 + blocks,)),
            pltpu.SemaphoreType.DMA((4,)),
        ],
        cost_estimate=pl.CostEstimate(
            flops=6 * groups * BLK * top * BLK * DH, transcendentals=groups * BLK * top * BLK, bytes_accessed=5 << 20
        ),
        name="memory_part",
    )(slots, tiles, q, gm, lq, own, back)


def join_kernel(pieces, *refs):
    outs = 1 + max(piece[0] for piece in pieces)
    sources, targets, stages, (taken, given) = (
        refs[: -2 * outs - 2],
        refs[-2 * outs - 2 : -outs - 2],
        refs[-outs - 2 : -2],
        refs[-2:],
    )
    count = [0] * outs
    steps = []
    for i, (out, source, row) in enumerate(pieces):
        rows = stages[out].shape[0] // sum(piece[0] == out for piece in pieces)
        here = pl.ds(count[out] * rows, rows)
        count[out] += 1
        steps.append(
            (
                pltpu.make_async_copy(sources[source].at[pl.ds(row, rows)], stages[out].at[here], taken.at[i]),
                pltpu.make_async_copy(stages[out].at[here], targets[out].at[here], given.at[i]),
            )
        )
    for take, _ in steps:
        take.start()
    for take, give in steps:
        take.wait()
        give.start()
    for _, give in steps:
        give.wait()


def join(pieces, sources, rows):
    width = sources[0].shape[1]
    shapes = [(n, width) for n in rows]
    return pl.pallas_call(
        functools.partial(join_kernel, tuple(pieces)),
        out_shape=tuple(jax.ShapeDtypeStruct(shape, BF16) for shape in shapes),
        in_specs=[HBM] * len(sources),
        out_specs=(HBM,) * len(rows),
        scratch_shapes=[pltpu.VMEM(shape, BF16) for shape in shapes]
        + [pltpu.SemaphoreType.DMA((len(pieces),)), pltpu.SemaphoreType.DMA((len(pieces),))],
        name="join",
    )(*sources)


def head_kernel(order, go_a, go_b, w_a, w_b, out):
    part = dot_nn(
        jnp.concatenate([go_a[...], go_b[...]], axis=1), jnp.concatenate([w_a[...], w_b[...]], axis=0)
    )

    @pl.when(pl.program_id(0) == 0)
    def _():
        out[...] = part

    @pl.when(pl.program_id(0) > 0)
    def _():
        out[...] += part


def head_part(order, grad_out, w_a, w_b):
    tokens = grad_out.shape[0]
    rows, width = w_a.shape
    steps = rows // BLK
    return pl.pallas_call(
        head_kernel,
        grid_spec=pltpu.PrefetchScalarGridSpec(
            num_scalar_prefetch=1,
            grid=(steps,),
            in_specs=[
                pl.BlockSpec((tokens, BLK), lambda k, order: (0, order[0, k])),
                pl.BlockSpec((tokens, BLK), lambda k, order: (0, order[1, k])),
                pl.BlockSpec((BLK, width), lambda k, order: (k, 0)),
                pl.BlockSpec((BLK, width), lambda k, order: (k, 0)),
            ],
            out_specs=pl.BlockSpec((tokens, width), lambda k, order: (0, 0)),
        ),
        out_shape=jax.ShapeDtypeStruct((tokens, width), F32),
        cost_estimate=pl.CostEstimate(
            flops=4 * tokens * rows * width, transcendentals=0, bytes_accessed=9 << 20
        ),
        name="head_part",
    )(order, grad_out, grad_out, w_a, w_b)


def local_kernel(scale, window, start, gate, q, k, v, hk, hv, hg, gm_out, lq_out, own_out, back_out):
    head = pl.program_id(0)
    share = gate[head]
    blocks = q.shape[0] // BLK
    tail = q.shape[0] - 2 * BLK
    key_blocks = [hk[tail : tail + BLK], hk[tail + BLK :]] + [k[i * BLK : (i + 1) * BLK] for i in range(blocks)]
    val_blocks = [hv[tail : tail + BLK], hv[tail + BLK :]] + [v[i * BLK : (i + 1) * BLK] for i in range(blocks)]
    key_sums = [None] * (blocks + 2)
    val_sums = [None] * (blocks + 2)
    row = lax.broadcasted_iota(jnp.int32, (BLK, 3 * BLK), 0)
    col = lax.broadcasted_iota(jnp.int32, (BLK, 3 * BLK), 1) - 2 * BLK
    for b in range(blocks):
        rows = slice(b * BLK, (b + 1) * BLK)
        grad = hg[rows, :]
        gm_out[rows, :] = (share * grad).astype(BF16)
        gl = ((1.0 - share) * grad).astype(BF16)
        qb = q[rows, :]
        keys = jnp.concatenate(key_blocks[b : b + 3], axis=0)
        vals = jnp.concatenate(val_blocks[b : b + 3], axis=0)
        allowed = (col <= row) & (col > row - window[b]) & (col + b * BLK >= -start[0])
        scores = jnp.where(allowed, dot_nt(qb, keys) * scale, -1e30)
        expo = jnp.exp(scores - jnp.max(scores, axis=-1, keepdims=True))
        probs = expo * (1.0 / jnp.sum(expo, axis=-1, keepdims=True))
        dprobs = dot_nt(gl, vals)
        delta = jnp.sum(probs * dprobs, axis=-1, keepdims=True)
        dscores = (probs * (dprobs - delta)).astype(BF16)
        probs16 = probs.astype(BF16)
        lq_out[rows, :] = dot_nn(dscores, keys) * scale
        key_grad = dot_tn(dscores, qb)
        val_grad = dot_tn(probs16, gl)
        for j in range(3):
            part = slice(j * BLK, (j + 1) * BLK)
            for sums, grads in ((key_sums, key_grad), (val_sums, val_grad)):
                sums[b + j] = grads[part] if sums[b + j] is None else sums[b + j] + grads[part]
    for i in range(2):
        back_out[0, i * BLK : (i + 1) * BLK, :] = (key_sums[i] * scale).astype(BF16)
        back_out[1, i * BLK : (i + 1) * BLK, :] = val_sums[i].astype(BF16)
    for i in range(blocks):
        own_out[0, i * BLK : (i + 1) * BLK, :] = key_sums[i + 2] * scale
        own_out[1, i * BLK : (i + 1) * BLK, :] = val_sums[i + 2]


def local_part(window, start, gate, q, k, v, hk, hv, hg, scale):
    tokens, width = q.shape
    heads = width // DH
    column = pl.BlockSpec((tokens, DH), lambda h: (0, h))
    pair = pl.BlockSpec((2, 2 * BLK, DH), lambda h: (0, 0, h))
    both = pl.BlockSpec((2, tokens, DH), lambda h: (0, 0, h))
    return pl.pallas_call(
        functools.partial(local_kernel, scale),
        grid=(heads,),
        out_shape=(
            jax.ShapeDtypeStruct((tokens, width), BF16),
            jax.ShapeDtypeStruct((tokens, width), F32),
            jax.ShapeDtypeStruct((2, tokens, width), F32),
            jax.ShapeDtypeStruct((2, 2 * BLK, width), BF16),
        ),
        in_specs=[SMEM, SMEM, SMEM, column, column, column, column, column, column],
        out_specs=(column, column, both, pair),
        cost_estimate=pl.CostEstimate(
            flops=10 * tokens * 3 * BLK * width, transcendentals=tokens * 3 * BLK * heads, bytes_accessed=6 << 20
        ),
        name="local_part",
    )(window, start, gate, q, k, v, hk, hv, hg)


def place_of(x, y, core):
    return (x % 4) * 8 + (y % 4) * 2 + core


def torus(shift, phase):
    pairs = []
    for x in range(4):
        for y in range(4):
            for core in range(2):
                dx, dy = (shift, 0) if core == phase else (0, shift)
                pairs.append((place_of(x, y, core), place_of(x + dx, y + dy, core)))
    return pairs


def arrival(me):
    x, y, core = me >> 3, (me >> 1) & 3, me & 1
    step = jnp.arange(16, dtype=jnp.int32)
    first, second = step & 3, step >> 2
    south = place_of(x - first, y - second, 0)
    north = place_of(x - second, y - first, 1)
    return jnp.where(core == 0, jnp.stack([south, north]), jnp.stack([north, south]))


def body(
    queries,
    local_keys,
    local_values,
    memory_keys,
    memory_values,
    grad_out,
    out_weight,
    gate_logits,
    tile_ids,
    window,
):
    _, heads, top = tile_ids.shape
    members = lax.axis_size("mem")
    me = lax.axis_index("mem")
    core = (me & 1).reshape(1)
    scale = 1.0 / math.sqrt(DH)
    tokens = queries.shape[0]

    onward = [(i, (i + 1) % members) for i in range(members)]
    halo_keys = lax.ppermute(local_keys, "mem", onward)
    halo_values = lax.ppermute(local_values, "mem", onward)

    request, slots = requests(tile_ids, members)
    codes = lax.all_to_all(request, "mem", split_axis=0, concat_axis=0, tiled=True)

    partner = [(i, i ^ 1) for i in range(members)]
    peer_keys = lax.ppermute(memory_keys, "mem", partner)
    peer_vals = lax.ppermute(memory_values, "mem", partner)
    rows = [out_weight] + [lax.ppermute(out_weight, "mem", torus(shift, 0)) for shift in (1, 2, 3)]
    sources = (codes, core, memory_keys, memory_values, peer_keys, peer_vals)
    sent = gather_tiles(*sources, 0, UNITS)
    (band,) = join([(0, i, 0) for i in range(4)], rows, (4 * out_weight.shape[0],))
    bands = [band] + [lax.ppermute(band, "mem", torus(shift, 1)) for shift in (1, 2, 3)]
    tiles = lax.all_to_all(sent, "mem", split_axis=0, concat_axis=0, tiled=True)

    (w_own,) = join([(0, i, 0) for i in range(4)], bands, (4 * band.shape[0],))
    w_peer = lax.ppermute(w_own, "mem", partner)
    head_grad = head_part(arrival(me), grad_out, w_own, w_peer)
    gate = jax.nn.sigmoid(gate_logits)
    start = (me * tokens).reshape(1)
    gm, lq, own, back = local_part(
        window, start, gate, queries, local_keys, local_values, halo_keys, halo_values, head_grad, scale
    )
    back = lax.ppermute(back, "mem", [(i + 1, i) for i in range(members - 1)])

    def usual():
        flat = tiles.reshape(members * UNITS, BLK, DH)
        return memory_part(slots, flat, queries, gm, lq, own, back, UNITS, heads, top, scale)

    def with_sixth():
        sixth = gather_tiles(*sources, UNITS, 1)
        sixth = lax.all_to_all(sixth, "mem", split_axis=0, concat_axis=0, tiled=True)
        flat = jnp.concatenate([tiles, sixth], axis=1).reshape(members * (UNITS + 1), BLK, DH)
        return memory_part(slots, flat, queries, gm, lq, own, back, UNITS + 1, heads, top, scale)

    return lax.cond(jnp.max(codes[:, 0, FLAG]) > 0, with_sixth, usual)


def solution(mesh):
    in_specs = (
        P("mem", "mp"),
        P("mem", "mp"),
        P("mem", "mp"),
        P("mem", "mp"),
        P("mem", "mp"),
        P("mem", None),
        P("mem", "mp"),
        P("mp"),
        P("mem", "mp", None),
        P("mem"),
    )
    out_specs = (P("mem", "mp"), P("mem", "mp"), P("mem", "mp"))

    return jax.shard_map(body, mesh=mesh, in_specs=in_specs, out_specs=out_specs, check_vma=False)
```
